32 devices in a mesh: morton: 8 (over z, x), level: 4 (over y, core).
Axes of the slice: x: 2, y: 2, z: 4, core: 2. Of those that a mesh axis runs over, the one named last changes fastest.
Arguments:
- coarse_density: float32 [4096, 128], P('morton'), may hold values from 0.000125 to 0.12
- coarse_emission: float32 [4096, 128], P('morton'), may hold values from 0 to 4
- fine_density: float32 [16384, 128], P(('morton', 'level')), may hold values from 0.000125 to 0.12
- fine_emission: float32 [16384, 128], P(('morton', 'level')), may hold values from 0 to 4
- coarse_brick: int32 [32768], P(('morton', 'level')), may hold values from 0 to 15
- coarse_lane: int32 [32768], P(('morton', 'level')), may hold values from 0 to 1023
- coarse_entry: int32 [32768], P(('morton', 'level')), may hold values from 0 to 31, as said below
- coarse_count: int32 [32768], P(('morton', 'level')), may hold values from 0 to 32, as said below
- fine_owner: int32 [262144, 1], P(('morton', 'level')), may hold values from 0 to 31; in each aligned block of 8192 rows (0 to 8191, 8192 to 16383, ...) at most 512 rows name the same one
- fine_brick: int32 [262144], P(('morton', 'level')), may hold values from 0 to 1
- fine_lane: int32 [262144], P(('morton', 'level')), may hold values from 0 to 1023
- fine_entry: int32 [262144], P(('morton', 'level')), may hold values from 0 to 31, as said below
- fine_count: int32 [262144], P(('morton', 'level')), may hold values from 0 to 32, as said below
Outputs:
- image_color: float32 [8192], P(('morton', 'level'))
- transmittance: float32 [8192], P(('morton', 'level'))
The draws below stay inside these ranges and needn't reach their ends.
Inputs may be any that keep to these rules, and one draw needn't show every extreme that they name: `coarse_entry`: entry plus count is at most 32 for each segment. `coarse_count`: count 0 marks an empty segment. `fine_entry`: entry plus count is at most 32 for each segment. `fine_count`: count 0 marks a padded slot. `fine_owner`: among the fine segments of one device, at most 512 name one owner device, a bound that some block reaches.
All inputs are finite; a program needn't handle non-finite values.
Results may differ from the reference program's by a relative error of at most 0.0003.
Values sent between devices are 32-bit elements; how exact they have to be, the bound alone decides.
A program may use at most 64 MiB of HBM per device.

```python
import math
import jax
import jax.numpy as jnp
import numpy as np
from jax import lax

BRICK = 32
BROWS = 256
FB = 2
CB = 16
GROUP_PIX = 1024
FSEG = 8
RCAP = 512
SLABSEG = 32768
SEGT = 262144
FINE = 64
N_MORTON = 8
N_LEVEL = 4


def entry_and_count(key, salt, total):
    inner = jax.random.fold_in(key, salt)
    first_key, second_key = jax.random.split(inner)
    entry_ids = jax.random.randint(first_key, (total,), 0, BRICK)
    count_ids = jax.random.randint(second_key, (total,), 0, BRICK - entry_ids + 1)
    return (entry_ids.astype(jnp.int32), count_ids.astype(jnp.int32))


def density_field(key, bricks):
    inner = jax.random.fold_in(key, 29)
    scale_key, cell_key = jax.random.split(inner)
    brick_scale = jnp.exp(jax.random.uniform(scale_key, (bricks, 1, 1), jnp.float32, math.log(0.0005), math.log(0.03)))
    cell_factor = jnp.exp(jax.random.uniform(cell_key, (bricks, BROWS, 128), jnp.float32, math.log(0.25), math.log(4.0)))
    return (brick_scale * cell_factor).reshape(bricks * BROWS, 128).astype(jnp.float32)


def draw_coarse_density(key, part):
    return density_field(key, CB)


def draw_fine_density(key, part):
    return density_field(key, FINE)


def draw_coarse_entry(key, part):
    return entry_and_count(key, 13, SLABSEG)[0]


def draw_coarse_count(key, part):
    return entry_and_count(key, 13, SLABSEG)[1]


def draw_fine_entry(key, part):
    return entry_and_count(key, 11, SEGT)[0]


def draw_fine_count(key, part):
    return entry_and_count(key, 11, SEGT)[1]


def touch_ends(drawn, stream_key, smallest, largest):
    place = [jax.random.randint(jax.random.fold_in(stream_key, axis), (), 0, length) for axis, length in enumerate(drawn.shape)]
    longest = drawn.shape.index(max(drawn.shape))
    beside = place[:longest] + [(place[longest] + 1) % drawn.shape[longest]] + place[longest + 1:]
    return drawn.at[tuple(place)].set(smallest).at[tuple(beside)].set(largest)


def steps_of(own_key, dims, shards, least, high):
    def one(axis_at, shards_of):
        heights = jax.random.uniform(jax.random.fold_in(jax.random.fold_in(own_key, 6), axis_at), (shards_of,), jnp.float32, least / len(shards), high / len(shards))
        return jnp.repeat(jnp.exp(heights), dims[axis_at] // shards_of).reshape((-1,) + (1,) * (len(dims) - axis_at - 1))

    factor_of = one(*shards[0])
    for cut in shards[1:]:
        factor_of = factor_of * one(*cut)
    return factor_of


def routed_block(stream_key, own, number, rows, amount, top, reach, lean):
    ranking = jax.random.permutation(stream_key, amount)
    crowded, common = shares(amount, rows * top, reach, lean, True), shares(amount, rows * top, reach, lean, False)
    places = jnp.arange(amount)

    def named(sizes, offset_by):
        used = int((sizes > 0).sum())
        fixed = max(1, used // 4)
        passed = fixed + (places - fixed + offset_by * (used - fixed)) % max(1, amount - fixed)
        return jnp.zeros((amount,), jnp.int32).at[ranking[jnp.where(places < fixed, places, passed)]].set(jnp.asarray(sizes, jnp.int32))

    sizes = jnp.where(number % 4 == 0, named(crowded, number // 4), named(common, number - number // 4 - 1))
    mixed = jax.random.permutation(jax.random.fold_in(own, 3), amount)
    giver, taker = mixed[0:amount // 2 * 2:2], mixed[1:amount // 2 * 2:2]
    slack = jnp.minimum(sizes[giver] - 1, reach - sizes[taker]) // 2
    slack = jnp.where((giver == ranking[0]) | (taker == ranking[0]) | (sizes[taker] == 0), 0, jnp.maximum(slack, 0))
    passed = jax.random.randint(jax.random.fold_in(own, 4), (amount // 2,), 0, 1 << 20) % (slack + 1)
    sizes = sizes.at[giver].add(-passed).at[taker].add(passed)
    items = jnp.searchsorted(jnp.cumsum(sizes), jnp.arange(rows * top), side="right").astype(jnp.int32)
    listing = items.reshape(top, rows).T
    listing = listing[jax.random.permutation(jax.random.fold_in(own, 1), rows)]
    offset_by = jax.random.randint(jax.random.fold_in(own, 2), (rows, 1), 0, top)
    return jnp.take_along_axis(listing, (jnp.arange(top)[None, :] + offset_by) % top, axis=1)


def shares(amount, total, bound, skew, full):
    loads = [(1 << 20) // math.isqrt(standing ** skew) + 1 for standing in range(1, amount + 1)]
    largest = bound if full else min(bound, max(-(-total // amount), total * loads[0] // sum(loads)))
    least = 1 if total - largest >= amount - 1 else 0
    counts, rest = [largest] + [least] * (amount - 1), total - largest - least * (amount - 1)
    while rest > 0:
        free = [i for i in range(1, amount) if counts[i] < largest] or [i for i in range(1, amount) if counts[i] < bound]
        whole, left = sum([loads[i] for i in free]), rest
        for i in free:
            addition = min(bound - counts[i], max(1, left * loads[i] // whole), rest)
            counts[i] = counts[i] + addition
            rest = rest - addition
    return np.array(counts)


def setup_inputs(seed: int = 0) -> dict:
    key_of = jax.random.split(jax.random.key(seed), 14)
    coarse_density = draw_coarse_density(jax.random.fold_in(key_of[13], 71), 0)
    coarse_emission = jnp.clip(4.0 * jax.random.uniform(key_of[1], (CB * BROWS, 128), jnp.float32) ** steps_of(key_of[1], (CB * BROWS, 128), ((0, 8),), -0.2, 0.2), 0.0, 4.0)
    fine_density = draw_fine_density(jax.random.fold_in(key_of[13], 71), 0)
    fine_emission = jnp.clip(4.0 * jax.random.uniform(key_of[3], (FINE * BROWS, 128), jnp.float32) ** steps_of(key_of[3], (FINE * BROWS, 128), ((0, 32),), -0.2, 0.2), 0.0, 4.0)
    coarse_brick = touch_ends(jax.random.randint(key_of[4], (SLABSEG,), 0, CB), jax.random.fold_in(key_of[4], 1), 0, CB - 1).astype(jnp.int32)
    coarse_lane = touch_ends(jax.random.randint(key_of[5], (SLABSEG,), 0, BRICK * BRICK), jax.random.fold_in(key_of[5], 1), 0, (BRICK * BRICK) - 1).astype(jnp.int32)
    coarse_entry = draw_coarse_entry(jax.random.fold_in(key_of[13], 71), 0)
    coarse_count = draw_coarse_count(jax.random.fold_in(key_of[13], 71), 0)
    fine_owner_keys = jax.random.split(jax.random.fold_in(key_of[8], 1), SEGT // (GROUP_PIX * FSEG))
    fine_owner_turns = jax.random.permutation(jax.random.fold_in(key_of[8], 3), SEGT // (GROUP_PIX * FSEG))
    fine_owner = jax.vmap(lambda own, number: routed_block(jax.random.fold_in(key_of[8], 2), own, number, GROUP_PIX * FSEG, N_MORTON * N_LEVEL, 1, RCAP, 2))(fine_owner_keys, fine_owner_turns).reshape((SEGT, 1))
    fine_brick = touch_ends(jax.random.randint(key_of[9], (SEGT,), 0, FB), jax.random.fold_in(key_of[9], 1), 0, FB - 1).astype(jnp.int32)
    fine_lane = touch_ends(jax.random.randint(key_of[10], (SEGT,), 0, BRICK * BRICK), jax.random.fold_in(key_of[10], 1), 0, (BRICK * BRICK) - 1).astype(jnp.int32)
    fine_entry = draw_fine_entry(jax.random.fold_in(key_of[13], 71), 0)
    fine_count = draw_fine_count(jax.random.fold_in(key_of[13], 71), 0)
    return {"coarse_density": coarse_density, "coarse_emission": coarse_emission, "fine_density": fine_density, "fine_emission": fine_emission, "coarse_brick": coarse_brick, "coarse_lane": coarse_lane, "coarse_entry": coarse_entry, "coarse_count": coarse_count, "fine_owner": fine_owner, "fine_brick": fine_brick, "fine_lane": fine_lane, "fine_entry": fine_entry, "fine_count": fine_count}


def march(density_rows, emission_rows, lane_ids, entry_ids, count_ids):
    per_row = 128 // BRICK
    chosen = ((lane_ids % per_row)[:, None] == lax.broadcasted_iota(jnp.int32, (1, per_row), 1))[:, :, None]
    nothing = jnp.float32(0.0)
    dens_lane = jnp.sum(jnp.where(chosen, density_rows.reshape(-1, per_row, BRICK), nothing), axis=1).T
    emis_lane = jnp.sum(jnp.where(chosen, emission_rows.reshape(-1, per_row, BRICK), nothing), axis=1).T
    step_ids = lax.broadcasted_iota(jnp.int32, (BRICK, 1), 0)
    inside = (step_ids >= entry_ids[None, :]) & (step_ids < (entry_ids + count_ids)[None, :])
    optical = jnp.where(inside, dens_lane, nothing)
    before = jnp.cumsum(optical, axis=0) - optical
    opacity = 1.0 - jnp.exp(-optical)
    colors = jnp.sum(jnp.exp(-before) * opacity * emis_lane, axis=0)
    return colors, jnp.sum(optical, axis=0)


def sample_table(dens_table, emis_table, brick_ids, lane_ids, entry_ids, count_ids):
    row_index = brick_ids * BROWS + lane_ids // (128 // BRICK)
    return march(dens_table[row_index], emis_table[row_index], lane_ids, entry_ids, count_ids)


def reference(coarse_density, coarse_emission, fine_density, fine_emission, coarse_brick, coarse_lane, coarse_entry, coarse_count, fine_owner, fine_brick, fine_lane, fine_entry, fine_count):
    groups = N_MORTON * N_LEVEL
    owner = fine_owner[:, 0]

    def one_slab(inputs):
        c_brick, c_lane, c_entry, c_count, f_owner, f_brick, f_lane, f_entry, f_count = inputs
        coarse_color, coarse_depth = sample_table(coarse_density, coarse_emission, c_brick, c_lane, c_entry, c_count)
        global_brick = f_owner * FB + f_brick
        seg_color, seg_depth = sample_table(fine_density, fine_emission, global_brick, f_lane, f_entry, f_count)
        seg_color = seg_color.reshape(GROUP_PIX, FSEG)
        seg_depth = seg_depth.reshape(GROUP_PIX, FSEG)
        earlier = jnp.cumsum(seg_depth, axis=1) - seg_depth
        slab_color = coarse_color + jnp.exp(-coarse_depth) * jnp.sum(jnp.exp(-earlier) * seg_color, axis=1)
        slab_depth = coarse_depth + jnp.sum(seg_depth, axis=1)
        return slab_color, slab_depth

    inputs = (coarse_brick.reshape(groups, GROUP_PIX), coarse_lane.reshape(groups, GROUP_PIX), coarse_entry.reshape(groups, GROUP_PIX), coarse_count.reshape(groups, GROUP_PIX), owner.reshape(groups, GROUP_PIX * FSEG), fine_brick.reshape(groups, GROUP_PIX * FSEG), fine_lane.reshape(groups, GROUP_PIX * FSEG), fine_entry.reshape(groups, GROUP_PIX * FSEG), fine_count.reshape(groups, GROUP_PIX * FSEG))
    slab_color, slab_depth = lax.map(one_slab, inputs)
    slab_color = slab_color.reshape(N_MORTON, N_LEVEL, GROUP_PIX)
    slab_depth = slab_depth.reshape(N_MORTON, N_LEVEL, GROUP_PIX)
    earlier = jnp.cumsum(slab_depth, axis=1) - slab_depth
    image_color = jnp.sum(jnp.exp(-earlier) * slab_color, axis=1).reshape(N_MORTON * GROUP_PIX)
    transmittance = jnp.exp(-jnp.sum(slab_depth, axis=1)).reshape(N_MORTON * GROUP_PIX)
    return image_color, transmittance
```

```python
import functools

import jax
import jax.numpy as jnp
from jax import lax
from jax.experimental import pallas as pl
from jax.experimental.pallas import tpu as pltpu
from jax.sharding import PartitionSpec as P

BRICK = 32
LANES = 128
PER_ROW = LANES // BRICK
BROWS = BRICK**3 // LANES
F32 = jnp.float32
BF16 = jnp.bfloat16
I32 = jnp.int32
CODE_BITS = 22
PRESENT = 1 << CODE_BITS
BLOCK = 512
VMEM = pl.BlockSpec(memory_space=pltpu.VMEM)
SMEM = pl.BlockSpec(memory_space=pltpu.SMEM)


def onehot(ids, width):
    rows = lax.broadcasted_iota(I32, (width, ids.shape[1]), 0)
    return jnp.where(rows == ids, 1.0, 0.0).astype(F32)


def split(x, parts):
    out = []
    for _ in range(parts):
        piece = x.astype(BF16)
        out.append(piece)
        x = x - piece.astype(F32)
    return out


def dot_nt(a, b):
    return lax.dot_general(a, b, (((1,), (1,)), ((), ())), preferred_element_type=F32)


def dot_nn(a, b):
    return jnp.dot(a, b, preferred_element_type=F32)


def rank_in(ones, upper, carry):
    within = dot_nn(ones.astype(BF16), upper)
    ranks = jnp.sum((within + carry) * ones, axis=0, keepdims=True)
    return ranks, carry + jnp.sum(ones, axis=1, keepdims=True)


def place(dest_ones, codes, slots, cap):
    pieces = [codes & 255, (codes >> 8) & 255, codes >> 16]
    left = jnp.concatenate([dest_ones * piece.astype(F32) for piece in pieces], axis=0)
    return dot_nt(left.astype(BF16), onehot(slots, cap).astype(BF16))


def join(placed, n):
    a, b, c = (placed[i * n : (i + 1) * n].astype(I32) for i in range(3))
    return a + (b << 8) + (c << 16)


def route_kernel(
    n_morton, n_level, cap_f, cap_c, fine_ref, coarse_ref, msg_ref, rank_ref, dest_ref, slot_ref, upper_ref
):
    n_dev = n_morton * n_level
    block = upper_ref.shape[0]
    upper_ref[...] = jnp.where(
        lax.broadcasted_iota(I32, (block, block), 0) < lax.broadcasted_iota(I32, (block, block), 1), 1.0, 0.0
    ).astype(BF16)
    depth, pixels = fine_ref.shape
    mask = PRESENT - 1

    def one_row(f, state):
        carry, placed = state
        for h in range(0, pixels, block):
            packed = fine_ref[pl.ds(f, 1), h : h + block]
            ones = onehot(packed >> CODE_BITS, n_dev)
            ranks, carry = rank_in(ones, upper_ref[...], carry)
            ranks = ranks.astype(I32)
            rank_ref[pl.ds(f, 1), h : h + block] = ranks
            placed = placed + place(ones, (packed & mask) | PRESENT, ranks, cap_f)
        return carry, placed

    state = (jnp.zeros((n_dev, 1), F32), jnp.zeros((3 * n_dev, cap_f), F32))
    _, placed = lax.fori_loop(0, depth, one_row, state)
    fine_msg = join(placed, n_dev)
    carry = jnp.zeros((n_morton, 1), F32)
    placed = jnp.zeros((3 * n_dev, cap_c), F32)
    for h in range(0, pixels, block):
        packed = coarse_ref[:, h : h + block]
        group = packed >> CODE_BITS
        ranks, carry = rank_in(onehot(group, n_morton), upper_ref[...], carry)
        slots = jnp.floor((ranks + 0.5) * (1.0 / n_level)).astype(I32)
        dest = group * n_level + (ranks.astype(I32) - slots * n_level)
        dest_ref[:, h : h + block] = dest
        slot_ref[:, h : h + block] = slots
        placed = placed + place(onehot(dest, n_dev), (packed & mask) | PRESENT, slots, cap_c)
    coarse_msg = join(placed, n_dev)
    for i in range(n_dev):
        msg_ref[i, :, :cap_f] = fine_msg[i : i + 1]
        msg_ref[i, :, cap_f:] = coarse_msg[i : i + 1]


def cells_of(shape):
    rows = lax.broadcasted_iota(I32, shape, 0)
    return (rows & -BRICK) + 4 * (rows & 7) + ((rows >> 3) & 3)


def serve_kernel(
    cap_f, flag_ref, code_ref, fd_ref, fe_ref, cd_ref, ce_ref, out_ref, ft_ref, ct_ref
):
    turn = jnp.where(
        cells_of((LANES, LANES)) == lax.broadcasted_iota(I32, (LANES, LANES), 1), 1.0, 0.0
    ).astype(BF16)
    for table_ref, dens_ref, emis_ref in ((ft_ref, fd_ref, fe_ref), (ct_ref, cd_ref, ce_ref)):
        rows = dens_ref.shape[0]
        for at, ref in ((0, dens_ref), (LANES, emis_ref)):
            for i, piece in enumerate(split(ref[...], 2)):
                table_ref[at : at + LANES, i * rows : (i + 1) * rows] = dot_nt(turn, piece).astype(BF16)
    n_dev, _, cap = code_ref.shape
    step = LANES

    def one_source(i, _):
        for b, at in enumerate(range(0, cap, step)):
            table_ref = ft_ref if at < cap_f else ct_ref

            @pl.when(flag_ref[i, b] != 0)
            def _():
                codes = code_ref[i, :, at : at + step]
                first = (codes >> 6) & 127
                last = first + (codes & 63)
                ones = onehot((codes & (PRESENT - 1)) >> 13, table_ref.shape[1] // 2).astype(BF16)
                got = dot_nn(table_ref[...], jnp.concatenate([ones, ones], axis=0))
                cells = cells_of((LANES, step))
                inside = (cells >= first) & (cells < last)
                dens = jnp.where(inside, got[:LANES], 0.0)
                emis = jnp.where(inside, got[LANES:], 0.0)
                dens = sum(dens[g * BRICK : (g + 1) * BRICK] for g in range(PER_ROW))
                emis = sum(emis[g * BRICK : (g + 1) * BRICK] for g in range(PER_ROW))
                trans = jnp.exp(-dens)
                color = (1.0 - trans) * emis
                c, t = color[24:32], trans[24:32]
                for k in (2, 1, 0):
                    tk = trans[8 * k : 8 * k + 8]
                    c = color[8 * k : 8 * k + 8] + tk * c
                    t = tk * t
                for shift in (1, 2, 4):
                    c = c + t * pltpu.roll(c, 8 - shift, 0)
                    t = t * pltpu.roll(t, 8 - shift, 0)
                out_ref[i, 0:1, at : at + step] = c[0:1]
                out_ref[i, 1:2, at : at + step] = t[0:1]

            @pl.when(flag_ref[i, b] == 0)
            def _():
                out_ref[i, :, at : at + step] = jnp.zeros((2, step), F32)

        return 0

    lax.fori_loop(0, n_dev, one_source, 0)


def look_up(left, ones, dest_ones, n):
    got = dot_nn(left, ones)
    vals = []
    for v in range(2):
        total = sum(got[(v * 3 + i) * n : (v * 3 + i + 1) * n] for i in range(3))
        vals.append(jnp.sum(total * dest_ones, axis=0, keepdims=True))
    return vals


def blend_kernel(cap_f, resp_ref, fine_ref, rank_ref, dest_ref, slot_ref, out_ref, fl_ref, cl_ref):
    n_dev, _, cap = resp_ref.shape
    depth, pixels = fine_ref.shape
    for v in range(2):
        full = resp_ref[:, v, :]
        for i, piece in enumerate(split(full, 3)):
            at = (v * 3 + i) * n_dev
            fl_ref[at : at + n_dev, :] = piece[:, :cap_f]
            cl_ref[at : at + n_dev, :] = piece[:, cap_f:]
    block = min(BLOCK, pixels)
    for h in range(0, pixels, block):
        c, t = look_up(
            cl_ref[...],
            onehot(slot_ref[:, h : h + block], cap - cap_f).astype(BF16),
            onehot(dest_ref[:, h : h + block], n_dev),
            n_dev,
        )

        def one_row(f, state):
            c, t = state
            fc, ft = look_up(
                fl_ref[...],
                onehot(rank_ref[pl.ds(f, 1), h : h + block], cap_f).astype(BF16),
                onehot(fine_ref[pl.ds(f, 1), h : h + block] >> CODE_BITS, n_dev),
                n_dev,
            )
            return c + t * fc, t * ft

        c, t = lax.fori_loop(0, depth, one_row, (c, t))
        out_ref[0:1, h : h + block] = c
        out_ref[1:2, h : h + block] = t


def shards(
    coarse_density,
    coarse_emission,
    fine_density,
    fine_emission,
    coarse_brick,
    coarse_lane,
    coarse_entry,
    coarse_count,
    fine_owner,
    fine_brick,
    fine_lane,
    fine_entry,
    fine_count,
):
    n_morton = lax.axis_size("morton")
    n_level = lax.axis_size("level")
    n_dev = n_morton * n_level
    segments = fine_brick.shape[0]
    pixels = coarse_brick.shape[0]
    per_pixel = segments // pixels
    cap_f = -(-(2 * segments // n_dev) // LANES) * LANES
    cap_c = -(-pixels // (n_level * LANES)) * LANES
    cap = cap_f + cap_c
    c_rows = coarse_density.shape[0]
    block = min(BLOCK, pixels)

    def pack(owner, row, lane, entry, count):
        code = (((row * PER_ROW + lane % PER_ROW) * BRICK + entry) << 6) + count
        return (owner << CODE_BITS) | code

    fine = pack(
        fine_owner[:, 0], fine_brick * BROWS + fine_lane // PER_ROW, fine_lane, fine_entry, fine_count
    )
    fine = fine.reshape(pixels, per_pixel).T
    row = coarse_brick * BROWS + coarse_lane // PER_ROW
    coarse = pack(row // c_rows, row % c_rows, coarse_lane, coarse_entry, coarse_count).reshape(1, pixels)
    msg, rank, dest, slot = pl.pallas_call(
        functools.partial(route_kernel, n_morton, n_level, cap_f, cap_c),
        out_shape=(
            jax.ShapeDtypeStruct((n_dev, 1, cap), I32),
            jax.ShapeDtypeStruct((per_pixel, pixels), I32),
            jax.ShapeDtypeStruct((1, pixels), I32),
            jax.ShapeDtypeStruct((1, pixels), I32),
        ),
        in_specs=[VMEM] * 2,
        out_specs=(VMEM,) * 4,
        scratch_shapes=[pltpu.VMEM((block, block), BF16)],
    )(fine, coarse)
    asked = lax.all_to_all(msg, ("morton", "level"), split_axis=0, concat_axis=0, tiled=True)
    flags = asked[:, 0, ::LANES]
    served = pl.pallas_call(
        functools.partial(serve_kernel, cap_f),
        out_shape=jax.ShapeDtypeStruct((n_dev, 2, cap), F32),
        in_specs=[SMEM] + [VMEM] * 5,
        out_specs=VMEM,
        scratch_shapes=[
            pltpu.VMEM((2 * LANES, 2 * fine_density.shape[0]), BF16),
            pltpu.VMEM((2 * LANES, 2 * c_rows), BF16),
        ],
    )(flags, asked, fine_density, fine_emission, coarse_density, coarse_emission)
    resp = lax.all_to_all(served, ("morton", "level"), split_axis=0, concat_axis=0, tiled=True)
    slab = pl.pallas_call(
        functools.partial(blend_kernel, cap_f),
        out_shape=jax.ShapeDtypeStruct((2, pixels), F32),
        in_specs=[VMEM] * 5,
        out_specs=VMEM,
        scratch_shapes=[pltpu.VMEM((6 * n_dev, cap_f), BF16), pltpu.VMEM((6 * n_dev, cap_c), BF16)],
    )(resp, fine, rank, dest, slot)
    quarter = pixels // n_level
    parts = slab.reshape(2, n_level, quarter).transpose(1, 0, 2)
    parts = lax.all_to_all(parts, "level", split_axis=0, concat_axis=0, tiled=True)
    color, trans = jnp.zeros((quarter,), F32), jnp.ones((quarter,), F32)
    for s in range(n_level):
        color = color + trans * parts[s, 0]
        trans = trans * parts[s, 1]
    return color, trans


def solution(mesh):
    both = P(("morton", "level"))
    rows = P(("morton", "level"), None)
    coarse = P("morton", None)
    return jax.shard_map(
        shards,
        mesh=mesh,
        in_specs=(coarse, coarse, rows, rows, both, both, both, both, rows, both, both, both, both),
        out_specs=(both, both),
        check_vma=False,
    )
```

```python
import functools

import jax
import jax.numpy as jnp
from jax import lax
from jax.experimental import pallas as pl
from jax.experimental.pallas import tpu as pltpu
from jax.sharding import PartitionSpec as P

BRICK = 32
LANES = 128
PER_ROW = LANES // BRICK
BROWS = BRICK**3 // LANES
F32 = jnp.float32
BF16 = jnp.bfloat16
I32 = jnp.int32
CODE_BITS = 22
PRESENT = 1 << CODE_BITS
BLOCK = 512
VMEM = pl.BlockSpec(memory_space=pltpu.VMEM)


def onehot(ids, width):
    rows = lax.broadcasted_iota(I32, (width, ids.shape[1]), 0)
    return jnp.where(rows == ids, 1.0, 0.0).astype(F32)


def split(x, parts):
    out = []
    for _ in range(parts):
        piece = x.astype(BF16)
        out.append(piece)
        x = x - piece.astype(F32)
    return out


def dot_nt(a, b):
    return lax.dot_general(a, b, (((1,), (1,)), ((), ())), preferred_element_type=F32)


def dot_nn(a, b):
    return jnp.dot(a, b, preferred_element_type=F32)


def rank_in(ones, upper, carry):
    within = dot_nn(ones.astype(BF16), upper)
    ranks = jnp.sum((within + carry) * ones, axis=0, keepdims=True)
    return ranks, carry + jnp.sum(ones, axis=1, keepdims=True)


def place(dest_ones, codes, slots, cap):
    pieces = [codes & 255, (codes >> 8) & 255, codes >> 16]
    left = jnp.concatenate([dest_ones * piece.astype(F32) for piece in pieces], axis=0)
    return dot_nt(left.astype(BF16), onehot(slots, cap).astype(BF16))


def join(placed, n):
    a, b, c = (placed[i * n : (i + 1) * n].astype(I32) for i in range(3))
    return a + (b << 8) + (c << 16)


def route_kernel(
    n_morton, n_level, cap_f, cap_c, fine_ref, coarse_ref, msg_ref, rank_ref, dest_ref, slot_ref, upper_ref
):
    n_dev = n_morton * n_level
    block = upper_ref.shape[0]
    upper_ref[...] = jnp.where(
        lax.broadcasted_iota(I32, (block, block), 0) < lax.broadcasted_iota(I32, (block, block), 1), 1.0, 0.0
    ).astype(BF16)
    depth, pixels = fine_ref.shape
    mask = PRESENT - 1

    def one_row(f, state):
        carry, placed = state
        for h in range(0, pixels, block):
            packed = fine_ref[pl.ds(f, 1), h : h + block]
            ones = onehot(packed >> CODE_BITS, n_dev)
            ranks, carry = rank_in(ones, upper_ref[...], carry)
            ranks = ranks.astype(I32)
            rank_ref[pl.ds(f, 1), h : h + block] = ranks
            placed = placed + place(ones, (packed & mask) | PRESENT, ranks, cap_f)
        return carry, placed

    state = (jnp.zeros((n_dev, 1), F32), jnp.zeros((3 * n_dev, cap_f), F32))
    _, placed = lax.fori_loop(0, depth, one_row, state)
    fine_msg = join(placed, n_dev)
    carry = jnp.zeros((n_morton, 1), F32)
    placed = jnp.zeros((3 * n_dev, cap_c), F32)
    for h in range(0, pixels, block):
        packed = coarse_ref[:, h : h + block]
        group = packed >> CODE_BITS
        ranks, carry = rank_in(onehot(group, n_morton), upper_ref[...], carry)
        slots = jnp.floor((ranks + 0.5) * (1.0 / n_level)).astype(I32)
        dest = group * n_level + (ranks.astype(I32) - slots * n_level)
        dest_ref[:, h : h + block] = dest
        slot_ref[:, h : h + block] = slots
        placed = placed + place(onehot(dest, n_dev), (packed & mask) | PRESENT, slots, cap_c)
    coarse_msg = join(placed, n_dev)
    for i in range(n_dev):
        msg_ref[i, :, :cap_f] = fine_msg[i : i + 1]
        msg_ref[i, :, cap_f:] = coarse_msg[i : i + 1]


def cells_of(shape):
    rows = lax.broadcasted_iota(I32, shape, 0)
    return (rows & -BRICK) + 4 * (rows & 7) + ((rows >> 3) & 3)


def serve_kernel(cap_f, code_ref, fd_ref, fe_ref, cd_ref, ce_ref, out_ref, ft_ref, ct_ref, *got_refs):
    turn = jnp.where(
        cells_of((LANES, LANES)) == lax.broadcasted_iota(I32, (LANES, LANES), 1), 1.0, 0.0
    ).astype(BF16)
    for table_ref, dens_ref, emis_ref in ((ft_ref, fd_ref, fe_ref), (ct_ref, cd_ref, ce_ref)):
        rows = dens_ref.shape[0]
        for at, ref in ((0, dens_ref), (LANES, emis_ref)):
            for i, piece in enumerate(split(ref[...], 2)):
                table_ref[at : at + LANES, i * rows : (i + 1) * rows] = dot_nt(turn, piece).astype(BF16)
    n_dev, _, cap = code_ref.shape

    def fetch(codes, table_ref, got_ref):
        ones = onehot((codes & (PRESENT - 1)) >> 13, table_ref.shape[1] // 2).astype(BF16)
        got_ref[...] = dot_nn(table_ref[...], jnp.concatenate([ones, ones], axis=0))

    def march(codes, got_ref, at):
        step = LANES
        first = (codes >> 6) & 127
        last = first + (codes & 63)
        cells = cells_of((LANES, step))
        inside = (cells >= first) & (cells < last)
        dens = jnp.where(inside, got_ref[:LANES, at : at + step], 0.0)
        emis = jnp.where(inside, got_ref[LANES:, at : at + step], 0.0)
        dens = sum(dens[g * BRICK : (g + 1) * BRICK] for g in range(PER_ROW))
        emis = sum(emis[g * BRICK : (g + 1) * BRICK] for g in range(PER_ROW))
        trans = jnp.exp(-dens)
        color = (1.0 - trans) * emis
        c, t = color[24:32], trans[24:32]
        for k in (2, 1, 0):
            tk = trans[8 * k : 8 * k + 8]
            c = color[8 * k : 8 * k + 8] + tk * c
            t = tk * t
        for shift in (1, 2, 4):
            c = c + t * pltpu.roll(c, 8 - shift, 0)
            t = t * pltpu.roll(t, 8 - shift, 0)
        return c[0:1], t[0:1]

    def put(i, at, c, t):
        out_ref[i, 0:1, at : at + LANES] = c
        out_ref[i, 1:2, at : at + LANES] = t

    tail = cap > cap_f + LANES
    group = len(got_refs) - 1

    def some_sources(j, _):
        for u in range(group):
            fetch(code_ref[group * j + u, :, :cap_f], ft_ref, got_refs[u])
        near = [code_ref[group * j + u, :, cap_f : cap_f + LANES] for u in range(group)]
        fetch(jnp.concatenate(near, axis=1), ct_ref, got_refs[group])
        for u in range(group):
            for at in range(0, cap_f, LANES):
                codes = code_ref[group * j + u, :, at : at + LANES]
                put(group * j + u, at, *march(codes, got_refs[u], at))
        for u in range(group):
            put(group * j + u, cap_f, *march(near[u], got_refs[group], u * LANES))
        return 0

    lax.fori_loop(0, n_dev // group, some_sources, 0)
    if tail:
        used = jnp.max(code_ref[:, 0, cap_f + LANES :]) > 0

        @pl.when(used)
        def _():
            def one_source(i, _):
                for at in range(cap_f + LANES, cap, LANES):
                    codes = code_ref[i, :, at : at + LANES]
                    got_ref = got_refs[group].at[:, :LANES]
                    fetch(codes, ct_ref, got_ref)
                    put(i, at, *march(codes, got_ref, 0))
                return 0

            lax.fori_loop(0, n_dev, one_source, 0)

        @pl.when(jnp.logical_not(used))
        def _():
            out_ref[:, :, cap_f + LANES :] = jnp.zeros((n_dev, 2, cap - cap_f - LANES), F32)


def exchange_kernel(n_level, x_ref, out_ref, send_sem, recv_sem, own_sem):
    n_dev = x_ref.shape[0]
    me = lax.axis_index("morton") * n_level + lax.axis_index("level")

    def target(k):
        to = lax.rem(me + k, n_dev)
        return to, (to // n_level, lax.rem(to, n_level))

    def remote(k):
        to, device = target(k)
        return pltpu.make_async_remote_copy(
            src_ref=x_ref.at[to],
            dst_ref=out_ref.at[me],
            send_sem=send_sem.at[k],
            recv_sem=recv_sem.at[k],
            device_id=device,
            device_id_type=pl.DeviceIdType.MESH,
        )

    barrier = pltpu.get_barrier_semaphore()

    def greet(k, _):
        pl.semaphore_signal(barrier, inc=1, device_id=target(k)[1], device_id_type=pl.DeviceIdType.MESH)
        return 0

    lax.fori_loop(1, n_dev, greet, 0)
    own = pltpu.make_async_copy(x_ref.at[me], out_ref.at[me], own_sem)
    own.start()
    pl.semaphore_wait(barrier, n_dev - 1)

    def send(k, _):
        remote(k).start()
        return 0

    lax.fori_loop(1, n_dev, send, 0)
    own.wait()

    def finish(k, _):
        remote(k).wait()
        return 0

    lax.fori_loop(1, n_dev, finish, 0)


def exchange(x, n_level, number):
    n_dev = x.shape[0]
    return pl.pallas_call(
        functools.partial(exchange_kernel, n_level),
        out_shape=jax.ShapeDtypeStruct(x.shape, x.dtype),
        in_specs=[VMEM],
        out_specs=VMEM,
        scratch_shapes=[
            pltpu.SemaphoreType.DMA((n_dev,)),
            pltpu.SemaphoreType.DMA((n_dev,)),
            pltpu.SemaphoreType.DMA,
        ],
        compiler_params=pltpu.CompilerParams(collective_id=number, has_side_effects=True),
    )(x)


def join_levels_kernel(n_level, x_ref, color_ref, trans_ref, land_ref, send_sem, recv_sem):
    group, me = lax.axis_index("morton"), lax.axis_index("level")
    barrier = pltpu.get_barrier_semaphore()
    for k in range(1, n_level):
        pl.semaphore_signal(
            barrier, inc=1, device_id=(group, lax.rem(me + k, n_level)), device_id_type=pl.DeviceIdType.MESH
        )
    pl.semaphore_wait(barrier, n_level - 1)
    copies = []
    for k in range(1, n_level):
        to = lax.rem(me + k, n_level)
        copies.append(
            pltpu.make_async_remote_copy(
                src_ref=x_ref.at[to],
                dst_ref=land_ref.at[me],
                send_sem=send_sem.at[k],
                recv_sem=recv_sem.at[k],
                device_id=(group, to),
                device_id_type=pl.DeviceIdType.MESH,
            )
        )
        copies[-1].start()
    land_ref[me] = x_ref[me]
    for copy in copies:
        copy.wait()
    color, trans = land_ref[0, 0:1, :], land_ref[0, 1:2, :]
    for s in range(1, n_level):
        color = color + trans * land_ref[s, 0:1, :]
        trans = trans * land_ref[s, 1:2, :]
    color_ref[...] = color
    trans_ref[...] = trans


def look_up(left, ones, dest_ones, n):
    got = dot_nn(left, ones)
    vals = []
    for v in range(2):
        total = sum(got[(v * 3 + i) * n : (v * 3 + i + 1) * n] for i in range(3))
        vals.append(jnp.sum(total * dest_ones, axis=0, keepdims=True))
    return vals


def blend_kernel(cap_f, resp_ref, fine_ref, rank_ref, dest_ref, slot_ref, out_ref, fl_ref, cl_ref):
    n_dev, _, cap = resp_ref.shape
    depth, pixels = fine_ref.shape
    for v in range(2):
        full = resp_ref[:, v, :]
        for i, piece in enumerate(split(full, 3)):
            at = (v * 3 + i) * n_dev
            fl_ref[at : at + n_dev, :] = piece[:, :cap_f]
            cl_ref[at : at + n_dev, :] = piece[:, cap_f:]
    block = min(BLOCK, pixels)
    for h in range(0, pixels, block):
        c, t = look_up(
            cl_ref[...],
            onehot(slot_ref[:, h : h + block], cap - cap_f).astype(BF16),
            onehot(dest_ref[:, h : h + block], n_dev),
            n_dev,
        )

        def one_row(f, state):
            c, t = state
            fc, ft = look_up(
                fl_ref[...],
                onehot(rank_ref[pl.ds(f, 1), h : h + block], cap_f).astype(BF16),
                onehot(fine_ref[pl.ds(f, 1), h : h + block] >> CODE_BITS, n_dev),
                n_dev,
            )
            return c + t * fc, t * ft

        c, t = lax.fori_loop(0, depth, one_row, (c, t))
        out_ref[0:1, h : h + block] = c
        out_ref[1:2, h : h + block] = t


def shards(
    coarse_density,
    coarse_emission,
    fine_density,
    fine_emission,
    coarse_brick,
    coarse_lane,
    coarse_entry,
    coarse_count,
    fine_owner,
    fine_brick,
    fine_lane,
    fine_entry,
    fine_count,
):
    n_morton = lax.axis_size("morton")
    n_level = lax.axis_size("level")
    n_dev = n_morton * n_level
    segments = fine_brick.shape[0]
    pixels = coarse_brick.shape[0]
    per_pixel = segments // pixels
    cap_f = -(-(2 * segments // n_dev) // LANES) * LANES
    cap_c = -(-pixels // (n_level * LANES)) * LANES
    cap = cap_f + cap_c
    c_rows = coarse_density.shape[0]
    block = min(BLOCK, pixels)

    def pack(owner, row, lane, entry, count):
        code = (((row * PER_ROW + lane % PER_ROW) * BRICK + entry) << 6) + count
        return (owner << CODE_BITS) | code

    fine = pack(
        fine_owner[:, 0], fine_brick * BROWS + fine_lane // PER_ROW, fine_lane, fine_entry, fine_count
    )
    fine = fine.reshape(pixels, per_pixel).T
    row = coarse_brick * BROWS + coarse_lane // PER_ROW
    coarse = pack(row // c_rows, row % c_rows, coarse_lane, coarse_entry, coarse_count).reshape(1, pixels)
    msg, rank, dest, slot = pl.pallas_call(
        functools.partial(route_kernel, n_morton, n_level, cap_f, cap_c),
        out_shape=(
            jax.ShapeDtypeStruct((n_dev, 1, cap), I32),
            jax.ShapeDtypeStruct((per_pixel, pixels), I32),
            jax.ShapeDtypeStruct((1, pixels), I32),
            jax.ShapeDtypeStruct((1, pixels), I32),
        ),
        in_specs=[VMEM] * 2,
        out_specs=(VMEM,) * 4,
        scratch_shapes=[pltpu.VMEM((block, block), BF16)],
    )(fine, coarse)
    asked = exchange(msg, n_level, 0)
    group = 2 if n_dev % 2 == 0 else 1
    served = pl.pallas_call(
        functools.partial(serve_kernel, cap_f),
        out_shape=jax.ShapeDtypeStruct((n_dev, 2, cap), F32),
        in_specs=[VMEM] * 5,
        out_specs=VMEM,
        scratch_shapes=[
            pltpu.VMEM((2 * LANES, 2 * fine_density.shape[0]), BF16),
            pltpu.VMEM((2 * LANES, 2 * c_rows), BF16),
        ]
        + [pltpu.VMEM((2 * LANES, cap_f), F32)] * group
        + [pltpu.VMEM((2 * LANES, group * LANES), F32)],
    )(asked, fine_density, fine_emission, coarse_density, coarse_emission)
    resp = exchange(served, n_level, 1)
    slab = pl.pallas_call(
        functools.partial(blend_kernel, cap_f),
        out_shape=jax.ShapeDtypeStruct((2, pixels), F32),
        in_specs=[VMEM] * 5,
        out_specs=VMEM,
        scratch_shapes=[pltpu.VMEM((6 * n_dev, cap_f), BF16), pltpu.VMEM((6 * n_dev, cap_c), BF16)],
    )(resp, fine, rank, dest, slot)
    quarter = pixels // n_level
    parts = slab.reshape(2, n_level, quarter).transpose(1, 0, 2)
    color, trans = pl.pallas_call(
        functools.partial(join_levels_kernel, n_level),
        out_shape=(jax.ShapeDtypeStruct((1, quarter), F32),) * 2,
        in_specs=[VMEM],
        out_specs=(VMEM,) * 2,
        scratch_shapes=[
            pltpu.VMEM((n_level, 2, quarter), F32),
            pltpu.SemaphoreType.DMA((n_level,)),
            pltpu.SemaphoreType.DMA((n_level,)),
        ],
        compiler_params=pltpu.CompilerParams(collective_id=2, has_side_effects=True),
    )(parts)
    return color.reshape(quarter), trans.reshape(quarter)


def solution(mesh):
    both = P(("morton", "level"))
    rows = P(("morton", "level"), None)
    coarse = P("morton", None)
    return jax.shard_map(
        shards,
        mesh=mesh,
        in_specs=(coarse, coarse, rows, rows, both, both, both, both, rows, both, both, both, both),
        out_specs=(both, both),
        check_vma=False,
    )
```

```python
import functools

import jax
import jax.numpy as jnp
from jax import lax
from jax.experimental import pallas as pl
from jax.experimental.pallas import tpu as pltpu
from jax.sharding import PartitionSpec as P

BRICK = 32
LANES = 128
PER_ROW = LANES // BRICK
BROWS = BRICK**3 // LANES
F32 = jnp.float32
BF16 = jnp.bfloat16
I32 = jnp.int32
CODE_BITS = 22
PRESENT = 1 << CODE_BITS
BLOCK = 512
VMEM = pl.BlockSpec(memory_space=pltpu.VMEM)


def onehot(ids, width):
    rows = lax.broadcasted_iota(I32, (width, ids.shape[1]), 0)
    return jnp.where(rows == ids, 1.0, 0.0).astype(F32)


def split(x, parts):
    out = []
    for _ in range(parts):
        piece = x.astype(BF16)
        out.append(piece)
        x = x - piece.astype(F32)
    return out


def dot_nt(a, b):
    return lax.dot_general(a, b, (((1,), (1,)), ((), ())), preferred_element_type=F32)


def dot_nn(a, b):
    return jnp.dot(a, b, preferred_element_type=F32)


def rank_in(ones, upper, carry):
    within = dot_nn(ones.astype(BF16), upper)
    ranks = jnp.sum((within + carry) * ones, axis=0, keepdims=True)
    return ranks, carry + jnp.sum(ones, axis=1, keepdims=True)


def place(dest_ones, codes, slots, cap):
    pieces = [codes & 255, (codes >> 8) & 255, codes >> 16]
    left = jnp.concatenate([dest_ones * piece.astype(F32) for piece in pieces], axis=0)
    return dot_nt(left.astype(BF16), onehot(slots, cap).astype(BF16))


def join(placed, n):
    a, b, c = (placed[i * n : (i + 1) * n].astype(I32) for i in range(3))
    return a + (b << 8) + (c << 16)


def paired_loop(steps, body, state):
    by = 2 if steps % 2 == 0 else 1

    def some(j, state):
        for u in range(by):
            state = body(by * j + u, state)
        return state

    return lax.fori_loop(0, steps // by, some, state)


def route(
    n_morton, n_level, cap_f, cap_c, fine_ref, coarse_ref, msg_ref, rank_ref, dest_ref, slot_ref, upper_ref
):
    n_dev = n_morton * n_level
    block = upper_ref.shape[0]
    upper_ref[...] = jnp.where(
        lax.broadcasted_iota(I32, (block, block), 0) < lax.broadcasted_iota(I32, (block, block), 1), 1.0, 0.0
    ).astype(BF16)
    depth, pixels = fine_ref.shape
    mask = PRESENT - 1

    def one_row(f, state):
        carry, placed = state
        for h in range(0, pixels, block):
            packed = fine_ref[pl.ds(f, 1), h : h + block]
            ones = onehot(packed >> CODE_BITS, n_dev)
            ranks, carry = rank_in(ones, upper_ref[...], carry)
            ranks = ranks.astype(I32)
            rank_ref[pl.ds(f, 1), h : h + block] = ranks
            placed = placed + place(ones, (packed & mask) | PRESENT, ranks, cap_f)
        return carry, placed

    state = (jnp.zeros((n_dev, 1), F32), jnp.zeros((3 * n_dev, cap_f), F32))
    _, placed = paired_loop(depth, one_row, state)
    fine_msg = join(placed, n_dev)
    carry = jnp.zeros((n_morton, 1), F32)
    placed = jnp.zeros((3 * n_dev, cap_c), F32)
    for h in range(0, pixels, block):
        packed = coarse_ref[:, h : h + block]
        group = packed >> CODE_BITS
        ranks, carry = rank_in(onehot(group, n_morton), upper_ref[...], carry)
        slots = jnp.floor((ranks + 0.5) * (1.0 / n_level)).astype(I32)
        dest = group * n_level + (ranks.astype(I32) - slots * n_level)
        dest_ref[:, h : h + block] = dest
        slot_ref[:, h : h + block] = slots
        placed = placed + place(onehot(dest, n_dev), (packed & mask) | PRESENT, slots, cap_c)
    coarse_msg = join(placed, n_dev)
    for i in range(n_dev):
        msg_ref[i, :, :cap_f] = fine_msg[i : i + 1]
        msg_ref[i, :, cap_f:] = coarse_msg[i : i + 1]


def cells_of(shape):
    rows = lax.broadcasted_iota(I32, shape, 0)
    return (rows & -BRICK) + 4 * (rows & 7) + ((rows >> 3) & 3)


def turn_tables(pairs):
    turn = jnp.where(
        cells_of((LANES, LANES)) == lax.broadcasted_iota(I32, (LANES, LANES), 1), 1.0, 0.0
    ).astype(BF16)
    for table_ref, dens_ref, emis_ref in pairs:
        rows = dens_ref.shape[0]
        for at, ref in ((0, dens_ref), (LANES, emis_ref)):
            for i, piece in enumerate(split(ref[...], 2)):
                table_ref[at : at + LANES, i * rows : (i + 1) * rows] = dot_nt(turn, piece).astype(BF16)


def fetch(codes, table_ref, got_ref):
    ones = onehot((codes & (PRESENT - 1)) >> 13, table_ref.shape[1] // 2).astype(BF16)
    got_ref[...] = dot_nn(table_ref[...], jnp.concatenate([ones, ones], axis=0))


def march(codes, got_ref, at):
    step = LANES
    first = (codes >> 6) & 127
    last = first + (codes & 63)
    cells = cells_of((LANES, step))
    inside = (cells >= first) & (cells < last)
    dens = jnp.where(inside, got_ref[:LANES, at : at + step], 0.0)
    emis = jnp.where(inside, got_ref[LANES:, at : at + step], 0.0)
    dens = sum(dens[g * BRICK : (g + 1) * BRICK] for g in range(PER_ROW))
    emis = sum(emis[g * BRICK : (g + 1) * BRICK] for g in range(PER_ROW))
    trans = jnp.exp(-dens)
    color = (1.0 - trans) * emis
    c, t = color[24:32], trans[24:32]
    for k in (2, 1, 0):
        tk = trans[8 * k : 8 * k + 8]
        c = color[8 * k : 8 * k + 8] + tk * c
        t = tk * t
    for shift in (1, 2, 4):
        c = c + t * pltpu.roll(c, 8 - shift, 0)
        t = t * pltpu.roll(t, 8 - shift, 0)
    return c[0:1], t[0:1]


def frame_kernel(
    n_morton,
    n_level,
    cap_f,
    cap_c,
    fine_ref,
    coarse_ref,
    fd_ref,
    fe_ref,
    cd_ref,
    ce_ref,
    out_ref,
    rank_ref,
    dest_ref,
    slot_ref,
    upper_ref,
    ft_ref,
    ct_ref,
    fl_ref,
    cl_ref,
    msg_ref,
    code_ref,
    served_ref,
    resp_ref,
    slab_ref,
    ask_send,
    ask_recv,
    tell_send,
    tell_recv,
    join_send,
    join_recv,
    *got_refs,
):
    n_dev = n_morton * n_level
    level = lax.axis_index("level")
    me = lax.axis_index("morton") * n_level + level
    mesh_ids = pl.DeviceIdType.MESH

    def device(d):
        return d // n_level, lax.rem(d, n_level)

    def after(k):
        return lax.rem(me + k, n_dev)

    def before(k):
        return lax.rem(me + n_dev - k, n_dev)

    def ask(k):
        to = after(k)
        return pltpu.make_async_remote_copy(
            src_ref=msg_ref.at[to],
            dst_ref=code_ref.at[me],
            send_sem=ask_send.at[k],
            recv_sem=ask_recv.at[k],
            device_id=device(to),
            device_id_type=mesh_ids,
        )

    def tell(k):
        to = before(k)
        return pltpu.make_async_remote_copy(
            src_ref=served_ref.at[to],
            dst_ref=resp_ref.at[me],
            send_sem=tell_send.at[k],
            recv_sem=tell_recv.at[k],
            device_id=device(to),
            device_id_type=mesh_ids,
        )

    def join(k):
        to = lax.rem(level + k, n_level)
        return pltpu.make_async_remote_copy(
            src_ref=slab_ref.at[to],
            dst_ref=out_ref.at[level],
            send_sem=join_send.at[k],
            recv_sem=join_recv.at[k],
            device_id=(lax.axis_index("morton"), to),
            device_id_type=mesh_ids,
        )

    barrier = pltpu.get_barrier_semaphore()

    def each(low, high, act):
        def body(k, _):
            act(k)
            return 0

        lax.fori_loop(low, high, body, 0)

    each(1, n_dev, lambda k: pl.semaphore_signal(barrier, inc=1, device_id=device(after(k)), device_id_type=mesh_ids))
    route(
        n_morton, n_level, cap_f, cap_c, fine_ref, coarse_ref, msg_ref, rank_ref, dest_ref, slot_ref, upper_ref
    )
    pl.semaphore_wait(barrier, n_dev - 1)
    each(1, n_dev, lambda k: ask(k).start())
    code_ref[me] = msg_ref[me]
    turn_tables(((ft_ref, fd_ref, fe_ref), (ct_ref, cd_ref, ce_ref)))
    group = len(got_refs) // 2

    def put(i, at, c, t):
        served_ref[i, 0:1, at : at + LANES] = c
        served_ref[i, 1:2, at : at + LANES] = t

    def some_sources(j, _):
        for u in range(group):

            @pl.when(group * j + u > 0)
            def _():
                ask(group * j + u).wait_recv()

            @pl.when(group * (j - 1) + u > 0)
            def _():
                tell(group * (j - 1) + u).start()

        at_source = [before(group * j + u) for u in range(group)]
        for u, i in enumerate(at_source):
            fetch(code_ref[i, :, :cap_f], ft_ref, got_refs[u])
            fetch(code_ref[i, :, cap_f:], ct_ref, got_refs[group + u])
        for u, i in enumerate(at_source):
            for at in range(0, cap_f, LANES):
                put(i, at, *march(code_ref[i, :, at : at + LANES], got_refs[u], at))
            for at in range(0, cap_c, LANES):
                codes = code_ref[i, :, cap_f + at : cap_f + at + LANES]
                put(i, cap_f + at, *march(codes, got_refs[group + u], at))
        return 0

    lax.fori_loop(0, n_dev // group, some_sources, 0)
    for u in range(group):
        if n_dev - group + u > 0:
            tell(n_dev - group + u).start()
    resp_ref[me] = served_ref[me]
    each(1, n_dev, lambda k: tell(k).wait_recv())
    blend(cap_f, resp_ref, fine_ref, rank_ref, dest_ref, slot_ref, slab_ref, fl_ref, cl_ref)
    for k in range(1, n_level):
        join(k).start()
    out_ref[level] = slab_ref[level]
    each(1, n_dev, lambda k: ask(k).wait_send())
    each(1, n_dev, lambda k: tell(k).wait_send())
    for k in range(1, n_level):
        join(k).wait()


def look_up(left, ones, dest_ones, n):
    got = dot_nn(left, ones)
    vals = []
    for v in range(2):
        total = sum(got[(v * 3 + i) * n : (v * 3 + i + 1) * n] for i in range(3))
        vals.append(jnp.sum(total * dest_ones, axis=0, keepdims=True))
    return vals


def blend(cap_f, resp_ref, fine_ref, rank_ref, dest_ref, slot_ref, out_ref, fl_ref, cl_ref):
    n_dev, _, cap = resp_ref.shape
    depth, pixels = fine_ref.shape
    for v in range(2):
        full = resp_ref[:, v, :]
        for i, piece in enumerate(split(full, 3)):
            at = (v * 3 + i) * n_dev
            fl_ref[at : at + n_dev, :] = piece[:, :cap_f]
            cl_ref[at : at + n_dev, :] = piece[:, cap_f:]
    block = min(BLOCK, pixels)
    for h in range(0, pixels, block):
        c, t = look_up(
            cl_ref[...],
            onehot(slot_ref[:, h : h + block], cap - cap_f).astype(BF16),
            onehot(dest_ref[:, h : h + block], n_dev),
            n_dev,
        )

        def one_row(f, state):
            c, t = state
            fc, ft = look_up(
                fl_ref[...],
                onehot(rank_ref[pl.ds(f, 1), h : h + block], cap_f).astype(BF16),
                onehot(fine_ref[pl.ds(f, 1), h : h + block] >> CODE_BITS, n_dev),
                n_dev,
            )
            return c + t * fc, t * ft

        c, t = paired_loop(depth, one_row, (c, t))
        quarter = out_ref.shape[2]
        for at in range(0, block, quarter):
            part = (h + at) // quarter
            out_ref[part, 0:1, :] = c[:, at : at + quarter]
            out_ref[part, 1:2, :] = t[:, at : at + quarter]


def shards(
    coarse_density,
    coarse_emission,
    fine_density,
    fine_emission,
    coarse_brick,
    coarse_lane,
    coarse_entry,
    coarse_count,
    fine_owner,
    fine_brick,
    fine_lane,
    fine_entry,
    fine_count,
):
    n_morton = lax.axis_size("morton")
    n_level = lax.axis_size("level")
    n_dev = n_morton * n_level
    segments = fine_brick.shape[0]
    pixels = coarse_brick.shape[0]
    per_pixel = segments // pixels
    cap_f = -(-(2 * segments // n_dev) // LANES) * LANES
    cap_c = -(-pixels // (n_level * LANES)) * LANES
    cap = cap_f + cap_c
    c_rows = coarse_density.shape[0]
    block = min(BLOCK, pixels)

    def pack(owner, row, lane, entry, count):
        code = (((row * PER_ROW + lane % PER_ROW) * BRICK + entry) << 6) + count
        return (owner << CODE_BITS) | code

    fine = pack(
        fine_owner[:, 0], fine_brick * BROWS + fine_lane // PER_ROW, fine_lane, fine_entry, fine_count
    )
    fine = fine.reshape(pixels, per_pixel).T
    row = coarse_brick * BROWS + coarse_lane // PER_ROW
    coarse = pack(row // c_rows, row % c_rows, coarse_lane, coarse_entry, coarse_count).reshape(1, pixels)
    quarter = pixels // n_level
    group = 2 if n_dev % 2 == 0 else 1
    rows = fine_density.shape[0]
    sems = [pltpu.SemaphoreType.DMA((n_dev,))] * 4 + [pltpu.SemaphoreType.DMA((n_level,))] * 2
    parts = pl.pallas_call(
        functools.partial(frame_kernel, n_morton, n_level, cap_f, cap_c),
        out_shape=jax.ShapeDtypeStruct((n_level, 2, quarter), F32),
        in_specs=[VMEM] * 6,
        out_specs=VMEM,
        scratch_shapes=[
            pltpu.VMEM((per_pixel, pixels), I32),
            pltpu.VMEM((1, pixels), I32),
            pltpu.VMEM((1, pixels), I32),
            pltpu.VMEM((block, block), BF16),
            pltpu.VMEM((2 * LANES, 2 * rows), BF16),
            pltpu.VMEM((2 * LANES, 2 * c_rows), BF16),
            pltpu.VMEM((6 * n_dev, cap_f), BF16),
            pltpu.VMEM((6 * n_dev, cap_c), BF16),
            pltpu.VMEM((n_dev, 1, cap), I32),
            pltpu.VMEM((n_dev, 1, cap), I32),
            pltpu.VMEM((n_dev, 2, cap), F32),
            pltpu.VMEM((n_dev, 2, cap), F32),
            pltpu.VMEM((n_level, 2, quarter), F32),
        ]
        + sems
        + [pltpu.VMEM((2 * LANES, cap_f), F32)] * group
        + [pltpu.VMEM((2 * LANES, cap_c), F32)] * group,
        compiler_params=pltpu.CompilerParams(collective_id=0, has_side_effects=True),
    )(fine, coarse, fine_density, fine_emission, coarse_density, coarse_emission)
    color, trans = parts[0, 0], parts[0, 1]
    for s in range(1, n_level):
        color = color + trans * parts[s, 0]
        trans = trans * parts[s, 1]
    return color, trans


def solution(mesh):
    both = P(("morton", "level"))
    rows = P(("morton", "level"), None)
    coarse = P("morton", None)
    return jax.shard_map(
        shards,
        mesh=mesh,
        in_specs=(coarse, coarse, rows, rows, both, both, both, both, rows, both, both, both, both),
        out_specs=(both, both),
        check_vma=False,
    )
```

```python
import functools

import jax
import jax.numpy as jnp
from jax import lax
from jax.experimental import pallas as pl
from jax.experimental.pallas import tpu as pltpu
from jax.sharding import PartitionSpec as P

BRICK = 32
LANES = 128
PER_ROW = LANES // BRICK
BROWS = BRICK**3 // LANES
F32 = jnp.float32
BF16 = jnp.bfloat16
I32 = jnp.int32
CODE_BITS = 22
PRESENT = 1 << CODE_BITS
BLOCK = 512
VMEM = pl.BlockSpec(memory_space=pltpu.VMEM)


def onehot(ids, width):
    rows = lax.broadcasted_iota(I32, (width, ids.shape[1]), 0)
    return jnp.where(rows == ids, 1.0, 0.0).astype(F32)


def split(x, parts):
    out = []
    for _ in range(parts):
        piece = x.astype(BF16)
        out.append(piece)
        x = x - piece.astype(F32)
    return out


def dot_nt(a, b):
    return lax.dot_general(a, b, (((1,), (1,)), ((), ())), preferred_element_type=F32)


def dot_nn(a, b):
    return jnp.dot(a, b, preferred_element_type=F32)


def rank_in(ones, upper, carry):
    within = dot_nn(ones.astype(BF16), upper)
    ranks = jnp.sum((within + carry) * ones, axis=0, keepdims=True)
    return ranks, carry + jnp.sum(ones, axis=1, keepdims=True)


def place(dest_ones, codes, slots, cap):
    pieces = [codes & 255, (codes >> 8) & 255, codes >> 16]
    left = jnp.concatenate([dest_ones * piece.astype(F32) for piece in pieces], axis=0)
    return dot_nt(left.astype(BF16), onehot(slots, cap).astype(BF16))


def join(placed, n):
    a, b, c = (placed[i * n : (i + 1) * n].astype(I32) for i in range(3))
    return a + (b << 8) + (c << 16)


def paired_loop(steps, body, state):
    by = 2 if steps % 2 == 0 else 1

    def some(j, state):
        for u in range(by):
            state = body(by * j + u, state)
        return state

    return lax.fori_loop(0, steps // by, some, state)


def route(
    n_morton, n_level, cap_f, cap_c, fine_ref, coarse_ref, msg_ref, rank_ref, dest_ref, slot_ref, upper_ref
):
    n_dev = n_morton * n_level
    block = upper_ref.shape[0]
    upper_ref[...] = jnp.where(
        lax.broadcasted_iota(I32, (block, block), 0) < lax.broadcasted_iota(I32, (block, block), 1), 1.0, 0.0
    ).astype(BF16)
    depth, pixels = fine_ref.shape
    mask = PRESENT - 1

    def one_row(f, state):
        carry, placed = state
        for h in range(0, pixels, block):
            packed = fine_ref[pl.ds(f, 1), h : h + block]
            ones = onehot(packed >> CODE_BITS, n_dev)
            ranks, carry = rank_in(ones, upper_ref[...], carry)
            ranks = ranks.astype(I32)
            rank_ref[pl.ds(f, 1), h : h + block] = ranks
            placed = placed + place(ones, (packed & mask) | PRESENT, ranks, cap_f)
        return carry, placed

    state = (jnp.zeros((n_dev, 1), F32), jnp.zeros((3 * n_dev, cap_f), F32))
    _, placed = paired_loop(depth, one_row, state)
    fine_msg = join(placed, n_dev)
    carry = jnp.zeros((n_morton, 1), F32)
    placed = jnp.zeros((3 * n_dev, cap_c), F32)
    for h in range(0, pixels, block):
        packed = coarse_ref[:, h : h + block]
        group = packed >> CODE_BITS
        ranks, carry = rank_in(onehot(group, n_morton), upper_ref[...], carry)
        slots = jnp.floor((ranks + 0.5) * (1.0 / n_level)).astype(I32)
        dest = group * n_level + (ranks.astype(I32) - slots * n_level)
        dest_ref[:, h : h + block] = dest
        slot_ref[:, h : h + block] = slots
        placed = placed + place(onehot(dest, n_dev), (packed & mask) | PRESENT, slots, cap_c)
    coarse_msg = join(placed, n_dev)
    for i in range(n_dev):
        msg_ref[i, :, :cap_f] = fine_msg[i : i + 1]
        msg_ref[i, :, cap_f:] = coarse_msg[i : i + 1]


def cells_of(shape):
    rows = lax.broadcasted_iota(I32, shape, 0)
    return (rows & -BRICK) + 4 * (rows & 7) + ((rows >> 3) & 3)


def turn_tables(pairs):
    turn = jnp.where(
        cells_of((LANES, LANES)) == lax.broadcasted_iota(I32, (LANES, LANES), 1), 1.0, 0.0
    ).astype(BF16)
    for table_ref, dens_ref, emis_ref in pairs:
        for at, ref in ((0, dens_ref), (LANES, emis_ref)):
            for i, piece in enumerate(split(ref[...], 2)):
                top = 2 * LANES * i + at
                table_ref[top : top + LANES, :] = dot_nt(turn, piece).astype(BF16)


def fetch(codes, table_ref, got_ref):
    ones = onehot((codes & (PRESENT - 1)) >> 13, table_ref.shape[1]).astype(BF16)
    both = dot_nn(table_ref[...], ones)
    got_ref[...] = both[: 2 * LANES] + both[2 * LANES :]


def march(codes, got_ref, at):
    step = LANES
    first = (codes >> 6) & 127
    last = first + (codes & 63)
    cells = cells_of((LANES, step))
    inside = (cells >= first) & (cells < last)
    dens = jnp.where(inside, got_ref[:LANES, at : at + step], 0.0)
    emis = jnp.where(inside, got_ref[LANES:, at : at + step], 0.0)
    dens = sum(dens[g * BRICK : (g + 1) * BRICK] for g in range(PER_ROW))
    emis = sum(emis[g * BRICK : (g + 1) * BRICK] for g in range(PER_ROW))
    trans = jnp.exp(-dens)
    color = (1.0 - trans) * emis
    c, t = color[24:32], trans[24:32]
    for k in (2, 1, 0):
        tk = trans[8 * k : 8 * k + 8]
        c = color[8 * k : 8 * k + 8] + tk * c
        t = tk * t
    for shift in (1, 2, 4):
        c = c + t * pltpu.roll(c, 8 - shift, 0)
        t = t * pltpu.roll(t, 8 - shift, 0)
    return c[0:1], t[0:1]


def frame_kernel(
    n_morton,
    n_level,
    cap_f,
    cap_c,
    fine_ref,
    coarse_ref,
    *refs,
):
    tables, (out_ref, *refs) = refs[:4], refs[4:]
    (
    rank_ref,
    dest_ref,
    slot_ref,
    upper_ref,
    ft_ref,
    ct_ref,
    fl_ref,
    cl_ref,
    msg_ref,
    code_ref,
    served_ref,
    resp_ref,
    slab_ref,
    ask_send,
    ask_recv,
    tell_send,
    tell_recv,
    join_send,
    join_recv,
    table_sems,
    *refs,
    ) = refs
    copies = [
        pltpu.make_async_copy(src, dst, table_sems.at[i]) for i, (src, dst) in enumerate(zip(tables, refs[:4]))
    ]
    fd_ref, fe_ref, cd_ref, ce_ref = refs[:4]
    got_refs = refs[4:]
    for copy in copies:
        copy.start()
    n_dev = n_morton * n_level
    level = lax.axis_index("level")
    me = lax.axis_index("morton") * n_level + level
    mesh_ids = pl.DeviceIdType.MESH

    def device(d):
        return d // n_level, lax.rem(d, n_level)

    def after(k):
        return lax.rem(me + k, n_dev)

    def before(k):
        return lax.rem(me + n_dev - k, n_dev)

    def ask(k):
        to = after(k)
        return pltpu.make_async_remote_copy(
            src_ref=msg_ref.at[to],
            dst_ref=code_ref.at[me],
            send_sem=ask_send.at[k],
            recv_sem=ask_recv.at[k],
            device_id=device(to),
            device_id_type=mesh_ids,
        )

    def tell(k):
        to = before(k)
        return pltpu.make_async_remote_copy(
            src_ref=served_ref.at[to],
            dst_ref=resp_ref.at[me],
            send_sem=tell_send.at[k],
            recv_sem=tell_recv.at[k],
            device_id=device(to),
            device_id_type=mesh_ids,
        )

    def join(k):
        to = lax.rem(level + k, n_level)
        return pltpu.make_async_remote_copy(
            src_ref=slab_ref.at[to],
            dst_ref=out_ref.at[level],
            send_sem=join_send.at[k],
            recv_sem=join_recv.at[k],
            device_id=(lax.axis_index("morton"), to),
            device_id_type=mesh_ids,
        )

    barrier = pltpu.get_barrier_semaphore()

    def each(low, high, act):
        def body(k, _):
            act(k)
            return 0

        lax.fori_loop(low, high, body, 0)

    each(1, n_dev, lambda k: pl.semaphore_signal(barrier, inc=1, device_id=device(after(k)), device_id_type=mesh_ids))
    route(
        n_morton, n_level, cap_f, cap_c, fine_ref, coarse_ref, msg_ref, rank_ref, dest_ref, slot_ref, upper_ref
    )
    pl.semaphore_wait(barrier, n_dev - 1)
    each(1, n_dev, lambda k: ask(k).start())
    code_ref[me] = msg_ref[me]
    for copy in copies:
        copy.wait()
    turn_tables(((ft_ref, fd_ref, fe_ref), (ct_ref, cd_ref, ce_ref)))
    def put(i, at, c, t):
        served_ref[i, 0:1, at : at + LANES] = c
        served_ref[i, 1:2, at : at + LANES] = t

    def fetch_source(i, bufs):
        fetch(code_ref[i, :, :cap_f], ft_ref, bufs[0])
        fetch(code_ref[i, :, cap_f:], ct_ref, bufs[1])

    def march_source(i, bufs):
        for at in range(0, cap_f, LANES):
            put(i, at, *march(code_ref[i, :, at : at + LANES], bufs[0], at))
        for at in range(0, cap_c, LANES):
            put(i, cap_f + at, *march(code_ref[i, :, cap_f + at : cap_f + at + LANES], bufs[1], at))

    even, odd = got_refs[:2], got_refs[2:]
    for ref in odd:
        ref[...] = jnp.zeros(ref.shape, F32)

    def two_sources(j, _):
        for u in range(2):

            @pl.when(2 * j + u > 0)
            def _():
                ask(2 * j + u).wait_recv()

            @pl.when(2 * j - 3 + u > 0)
            def _():
                tell(2 * j - 3 + u).start()

        now, later = before(2 * j), before(2 * j + 1)
        fetch_source(now, even)
        march_source(before(jnp.maximum(2 * j - 1, 0)), odd)
        fetch_source(later, odd)
        march_source(now, even)
        return 0

    lax.fori_loop(0, n_dev // 2, two_sources, 0)
    for k in (n_dev - 3, n_dev - 2):
        if k > 0:
            tell(k).start()
    march_source(before(n_dev - 1), odd)
    tell(n_dev - 1).start()
    resp_ref[me] = served_ref[me]
    each(1, n_dev, lambda k: tell(k).wait_recv())
    blend(cap_f, resp_ref, fine_ref, rank_ref, dest_ref, slot_ref, slab_ref, fl_ref, cl_ref)
    for k in range(1, n_level):
        join(k).start()
    out_ref[level] = slab_ref[level]
    each(1, n_dev, lambda k: ask(k).wait_send())
    each(1, n_dev, lambda k: tell(k).wait_send())
    for k in range(1, n_level):
        join(k).wait()


def look_up(left, ones, dest_ones, n):
    got = dot_nn(left, ones)
    vals = []
    for v in range(2):
        total = sum(got[(v * 3 + i) * n : (v * 3 + i + 1) * n] for i in range(3))
        vals.append(jnp.sum(total * dest_ones, axis=0, keepdims=True))
    return vals


def blend(cap_f, resp_ref, fine_ref, rank_ref, dest_ref, slot_ref, out_ref, fl_ref, cl_ref):
    n_dev, _, cap = resp_ref.shape
    depth, pixels = fine_ref.shape
    for v in range(2):
        full = resp_ref[:, v, :]
        for i, piece in enumerate(split(full, 3)):
            at = (v * 3 + i) * n_dev
            fl_ref[at : at + n_dev, :] = piece[:, :cap_f]
            cl_ref[at : at + n_dev, :] = piece[:, cap_f:]
    block = min(BLOCK, pixels)
    for h in range(0, pixels, block):
        c, t = look_up(
            cl_ref[...],
            onehot(slot_ref[:, h : h + block], cap - cap_f).astype(BF16),
            onehot(dest_ref[:, h : h + block], n_dev),
            n_dev,
        )

        def one_row(f, state):
            c, t = state
            fc, ft = look_up(
                fl_ref[...],
                onehot(rank_ref[pl.ds(f, 1), h : h + block], cap_f).astype(BF16),
                onehot(fine_ref[pl.ds(f, 1), h : h + block] >> CODE_BITS, n_dev),
                n_dev,
            )
            return c + t * fc, t * ft

        c, t = paired_loop(depth, one_row, (c, t))
        quarter = out_ref.shape[2]
        for at in range(0, block, quarter):
            part = (h + at) // quarter
            out_ref[part, 0:1, :] = c[:, at : at + quarter]
            out_ref[part, 1:2, :] = t[:, at : at + quarter]


def shards(
    coarse_density,
    coarse_emission,
    fine_density,
    fine_emission,
    coarse_brick,
    coarse_lane,
    coarse_entry,
    coarse_count,
    fine_owner,
    fine_brick,
    fine_lane,
    fine_entry,
    fine_count,
):
    n_morton = lax.axis_size("morton")
    n_level = lax.axis_size("level")
    n_dev = n_morton * n_level
    segments = fine_brick.shape[0]
    pixels = coarse_brick.shape[0]
    per_pixel = segments // pixels
    cap_f = -(-(2 * segments // n_dev) // LANES) * LANES
    cap_c = -(-pixels // (n_level * LANES)) * LANES
    cap = cap_f + cap_c
    c_rows = coarse_density.shape[0]
    block = min(BLOCK, pixels)

    def pack(owner, row, lane, entry, count):
        code = (((row * PER_ROW + lane % PER_ROW) * BRICK + entry) << 6) + count
        return (owner << CODE_BITS) | code

    fine = pack(
        fine_owner[:, 0], fine_brick * BROWS + fine_lane // PER_ROW, fine_lane, fine_entry, fine_count
    )
    fine = fine.reshape(pixels, per_pixel).T
    row = coarse_brick * BROWS + coarse_lane // PER_ROW
    coarse = pack(row // c_rows, row % c_rows, coarse_lane, coarse_entry, coarse_count).reshape(1, pixels)
    quarter = pixels // n_level
    rows = fine_density.shape[0]
    sems = [pltpu.SemaphoreType.DMA((n_dev,))] * 4 + [pltpu.SemaphoreType.DMA((n_level,))] * 2
    parts = pl.pallas_call(
        functools.partial(frame_kernel, n_morton, n_level, cap_f, cap_c),
        out_shape=jax.ShapeDtypeStruct((n_level, 2, quarter), F32),
        in_specs=[VMEM] * 2 + [pl.BlockSpec(memory_space=pl.ANY)] * 4,
        out_specs=VMEM,
        scratch_shapes=[
            pltpu.VMEM((per_pixel, pixels), I32),
            pltpu.VMEM((1, pixels), I32),
            pltpu.VMEM((1, pixels), I32),
            pltpu.VMEM((block, block), BF16),
            pltpu.VMEM((4 * LANES, rows), BF16),
            pltpu.VMEM((4 * LANES, c_rows), BF16),
            pltpu.VMEM((6 * n_dev, cap_f), BF16),
            pltpu.VMEM((6 * n_dev, cap_c), BF16),
            pltpu.VMEM((n_dev, 1, cap), I32),
            pltpu.VMEM((n_dev, 1, cap), I32),
            pltpu.VMEM((n_dev, 2, cap), F32),
            pltpu.VMEM((n_dev, 2, cap), F32),
            pltpu.VMEM((n_level, 2, quarter), F32),
        ]
        + sems
        + [pltpu.SemaphoreType.DMA((4,))]
        + [pltpu.VMEM((rows, LANES), F32)] * 2
        + [pltpu.VMEM((c_rows, LANES), F32)] * 2
        + [pltpu.VMEM((2 * LANES, cap_f), F32), pltpu.VMEM((2 * LANES, cap_c), F32)] * 2,
        compiler_params=pltpu.CompilerParams(collective_id=0, has_side_effects=True),
    )(fine, coarse, fine_density, fine_emission, coarse_density, coarse_emission)
    color, trans = parts[0, 0], parts[0, 1]
    for s in range(1, n_level):
        color = color + trans * parts[s, 0]
        trans = trans * parts[s, 1]
    return color, trans


def solution(mesh):
    both = P(("morton", "level"))
    rows = P(("morton", "level"), None)
    coarse = P("morton", None)
    return jax.shard_map(
        shards,
        mesh=mesh,
        in_specs=(coarse, coarse, rows, rows, both, both, both, both, rows, both, both, both, both),
        out_specs=(both, both),
        check_vma=False,
    )
```
